32 devices in a mesh: ya: 8 (over z, y), zb: 4 (over x, core).
Axes of the slice: x: 2, y: 2, z: 4, core: 2. Of those that a mesh axis runs over, the one named last changes fastest.
Arguments:
- source: float32 [128, 128, 512], P(None, 'ya', 'zb'), may hold values from -6 to 6
- symbol_x: float32 [128], replicated, may hold values from 0.3 to 3
- symbol_y: float32 [128], replicated, may hold values from 0.3 to 3
- symbol_z: float32 [512], replicated, may hold values from 0.3 to 3
Outputs:
- modes: float32 [128, 128, 512], P('ya', 'zb')
The draws below stay inside these ranges and needn't reach their ends.
All inputs are finite; a program needn't handle non-finite values.
Results may differ from the reference program's by a relative error of at most 0.000071.
Values sent between devices are 32-bit elements; how exact they have to be, the bound alone decides.
A program may use at most 64 MiB of HBM per device.

```python
import jax
import jax.numpy as jnp
from jax import lax

GRID_X = 128
GRID_Y = 128
GRID_Z = 512


def block_levels(rng, shape, shards, low, top_value):
    def one(dim, parts):
        heights = jax.random.uniform(jax.random.fold_in(jax.random.fold_in(rng, 6), dim), (parts,), jnp.float32, low / len(shards), top_value / len(shards))
        return jnp.repeat(jnp.exp(heights), shape[dim] // parts).reshape((-1,) + (1,) * (len(shape) - dim - 1))

    gain = one(*shards[0])
    for cut in shards[1:]:
        gain = gain * one(*cut)
    return gain


def noise(rng, shape, width, limit, split=(), dtype=jnp.bfloat16):
    drawn = width * jax.random.normal(rng, shape, jnp.float32)
    if split:
        drawn = drawn * block_levels(rng, shape, split, -0.22, 0.18)
    return jnp.clip(drawn, -limit, limit).astype(dtype)


def setup_inputs(seed: int = 0) -> dict:
    splits = jax.random.split(jax.random.key(seed), 5)
    source = noise(splits[0], (GRID_X, GRID_Y, GRID_Z), 1.0, 6.0, ((1, 8), (2, 4)), jnp.float32)
    symbol_x = jnp.clip(jax.random.uniform(splits[1], (GRID_X,), jnp.float32, 0.3, 3.0), 0.3, 3.0)
    symbol_y = jnp.clip(jax.random.uniform(splits[2], (GRID_Y,), jnp.float32, 0.3, 3.0), 0.3, 3.0)
    symbol_z = jnp.clip(jax.random.uniform(splits[3], (GRID_Z,), jnp.float32, 0.3, 3.0), 0.3, 3.0)
    return {"source": source, "symbol_x": symbol_x, "symbol_y": symbol_y, "symbol_z": symbol_z}


def transform_table(count):
    rank = jnp.arange(count)
    angle = jnp.pi / (count + 1) * ((rank[:, None] + 1) * (rank[None, :] + 1) % (2 * count + 2)).astype(jnp.float32)
    return jnp.sin(angle) * (2.0 / (count + 1)) ** 0.5

def transform_dim(values, dim):
    moved = jnp.tensordot(values, transform_table(values.shape[dim]), axes=([dim], [0]), precision=lax.Precision.HIGHEST)
    return jnp.moveaxis(moved, -1, dim)

def reference(source, symbol_x, symbol_y, symbol_z):
    modes = source
    modes = transform_dim(modes, 0)
    modes = transform_dim(modes, 1)
    modes = transform_dim(modes, 2)
    symbol = symbol_x[:, None, None] + symbol_y[None, :, None] + symbol_z[None, None, :]
    modes = modes * lax.rsqrt(symbol)
    return modes
```

```python
import functools

import jax
import jax.numpy as jnp
import numpy as np
from jax import lax
from jax.experimental import pallas as pl
from jax.experimental.pallas import tpu as pltpu
from jax.sharding import PartitionSpec as P

MESH = pl.DeviceIdType.MESH
CHUNKS = 4


def transform_table(count):
    rank = np.arange(1, count + 1)
    angle = np.pi / (count + 1) * (rank[:, None] * rank[None, :] % (2 * count + 2))
    table = np.sqrt(2.0 / (count + 1)) * np.sin(angle)
    high = table.astype(jnp.bfloat16)
    low = (table - high.astype(np.float64)).astype(jnp.bfloat16)
    return high, low


def halves(values):
    high = values.astype(jnp.bfloat16)
    return high, (values - high.astype(jnp.float32)).astype(jnp.bfloat16)


def left_product(table3, values):
    high, low = halves(values)
    stacked = jnp.concatenate([high, low, high], axis=0)
    return jnp.dot(table3, stacked, preferred_element_type=jnp.float32)


def partner(me, step, count):
    if count & (count - 1):
        return lax.rem(me + step, count)
    flipped, bit = 0, 1
    while bit < count:
        flipped = flipped + lax.rem(me // bit + step // bit, 2) * bit
        bit *= 2
    return flipped


def back(me, step, count):
    if count & (count - 1):
        return lax.rem(me + count - step, count)
    return partner(me, step, count)


def kernel(
    n_ya, n_zb, chunks,
    source, table_x, table_y, high_z, low_z,
    out,
    src, tx, ty, hz, lz, first, second, third, lines,
    load_sem, send_a, recv_a, send_b, recv_b,
):
    ya, zb = lax.axis_index("ya"), lax.axis_index("zb")
    nx, yl, zl = source.shape
    ny = yl * n_ya
    kl = nx // n_ya
    jl = ny // n_zb
    nz = zl * n_zb
    kc = kl // chunks

    loads = [
        pltpu.make_async_copy(a, b, load_sem.at[i])
        for i, (a, b) in enumerate(
            [(source, src), (table_x, tx), (table_y, ty), (high_z, hz), (low_z, lz)]
        )
    ]
    for load in loads:
        load.start()

    barrier = pltpu.get_barrier_semaphore()

    def greet_a(step, _):
        pl.semaphore_signal(
            barrier, inc=1, device_id={"ya": partner(ya, step, n_ya)}, device_id_type=MESH
        )
        return 0

    def greet_b(step, _):
        pl.semaphore_signal(
            barrier, inc=1, device_id={"zb": partner(zb, step, n_zb)}, device_id_type=MESH
        )
        return 0

    lax.fori_loop(1, n_ya, greet_a, 0)
    lax.fori_loop(1, n_zb, greet_b, 0)

    loads[0].wait()
    loads[1].wait()

    flat_src = src.reshape(nx * yl, zl)
    flat_first = first.reshape(nx * yl, zl)

    def x_step(pair, _):
        values = jnp.concatenate(
            [flat_src[pl.ds(2 * pair + t, nx, stride=yl), :] for t in range(2)], axis=1
        )
        modes = left_product(tx[...], values)
        for t in range(2):
            flat_first[pl.ds(2 * pair + t, nx, stride=yl), :] = modes[:, t * zl:(t + 1) * zl]
        return 0

    lax.fori_loop(0, yl // 2, x_step, 0)

    pl.semaphore_wait(barrier, n_ya + n_zb - 2)

    def copy_a(chunk, step):
        peer = partner(ya, step, n_ya)
        return pltpu.make_async_remote_copy(
            src_ref=first.at[pl.ds(peer * kl + chunk * kc, kc)],
            dst_ref=second.at[pl.ds(chunk * kc, kc), pl.ds(pl.multiple_of(ya * yl, yl), yl)],
            send_sem=send_a.at[chunk, step],
            recv_sem=recv_a.at[chunk, step],
            device_id={"ya": peer},
            device_id_type=MESH,
        )

    def arrive_a(chunk, step):
        peer = back(ya, step, n_ya)
        there = second.at[pl.ds(chunk * kc, kc), pl.ds(pl.multiple_of(peer * yl, yl), yl)]
        return pltpu.make_async_copy(there, there, recv_a.at[chunk, step])

    def copy_b(chunk, step):
        peer = partner(zb, step, n_zb)
        return pltpu.make_async_remote_copy(
            src_ref=third.at[pl.ds(chunk * kc, kc), pl.ds(pl.multiple_of(peer * jl, jl), jl)],
            dst_ref=lines.at[zb, pl.ds(chunk * kc, kc)],
            send_sem=send_b.at[chunk, step],
            recv_sem=recv_b.at[chunk, step],
            device_id={"zb": peer},
            device_id_type=MESH,
        )

    def arrive_b(chunk, step):
        there = lines.at[back(zb, step, n_zb), pl.ds(chunk * kc, kc)]
        return pltpu.make_async_copy(there, there, recv_b.at[chunk, step])

    def each_a(todo):
        lax.fori_loop(1, n_ya, lambda i, _: (todo(n_ya - i), 0)[1], 0)

    def each_b(todo):
        lax.fori_loop(1, n_zb, lambda i, _: (todo(n_zb - i), 0)[1], 0)

    def send_chunk(chunk, _):
        each_a(lambda step: copy_a(chunk, step).start())
        return 0

    lax.fori_loop(0, chunks, send_chunk, 0)

    second[:, pl.ds(pl.multiple_of(ya * yl, yl), yl), :] = first[pl.ds(ya * kl, kl)]

    loads[2].wait()
    loads[3].wait()
    loads[4].wait()

    def y_stage(chunk):
        each_a(lambda step: arrive_a(chunk, step).wait())
        width = 2 if kc % 2 == 0 else 1
        for k in range(0, kc, width):
            values = jnp.concatenate(
                [second[chunk * kc + k + t] for t in range(width)], axis=1
            )
            modes = left_product(ty[...], values)
            for t in range(width):
                third[chunk * kc + k + t] = modes[:, t * zl:(t + 1) * zl]
        each_b(lambda step: copy_b(chunk, step).start())
        lines[zb, pl.ds(chunk * kc, kc)] = third[
            pl.ds(chunk * kc, kc), pl.ds(pl.multiple_of(zb * jl, jl), jl), :
        ]

    def z_stage(chunk):
        each_b(lambda step: arrive_b(chunk, step).wait())
        values = jnp.concatenate(
            [lines[b, pl.ds(chunk * kc, kc)].reshape(kc * jl, zl) for b in range(n_zb)], axis=1
        )
        high, low = halves(values)
        dot = functools.partial(jnp.dot, preferred_element_type=jnp.float32)
        modes = dot(high, hz[...]) + dot(low, hz[...]) + dot(high, lz[...])
        out[pl.ds(chunk * kc, kc)] = modes.reshape(kc, jl, nz)

    def both(chunk, _):
        y_stage(chunk)
        z_stage(chunk - 1)
        return 0

    y_stage(0)
    lax.fori_loop(1, chunks, both, 0)
    z_stage(chunks - 1)

    def drain(chunk, _):
        each_a(lambda step: copy_a(chunk, step).wait_send())
        each_b(lambda step: copy_b(chunk, step).wait_send())
        return 0

    lax.fori_loop(0, chunks, drain, 0)


def body(n_ya, n_zb, source, symbol_x, symbol_y, symbol_z):
    nx, yl, zl = source.shape
    ny, nz = yl * n_ya, zl * n_zb
    kl, jl = nx // n_ya, ny // n_zb
    chunks = min(CHUNKS, kl)
    tables = []
    for count in (nx, ny):
        high, low = transform_table(count)
        tables.append(np.concatenate([high, high, low], axis=1))
    tables += list(transform_table(nz))
    dma = pltpu.SemaphoreType.DMA
    vmem = pltpu.VMEM
    modes = pl.pallas_call(
        functools.partial(kernel, n_ya, n_zb, chunks),
        out_shape=jax.ShapeDtypeStruct((kl, jl, nz), jnp.float32),
        in_specs=[pl.BlockSpec(memory_space=pltpu.HBM)] * 5,
        out_specs=pl.BlockSpec(memory_space=pltpu.VMEM),
        scratch_shapes=[
            vmem((nx, yl, zl), jnp.float32),
            vmem((nx, 3 * nx), jnp.bfloat16),
            vmem((ny, 3 * ny), jnp.bfloat16),
            vmem((nz, nz), jnp.bfloat16),
            vmem((nz, nz), jnp.bfloat16),
            vmem((nx, yl, zl), jnp.float32),
            vmem((kl, ny, zl), jnp.float32),
            vmem((kl, ny, zl), jnp.float32),
            vmem((n_zb, kl, jl, zl), jnp.float32),
            dma((5,)),
            dma((chunks, n_ya)),
            dma((chunks, n_ya)),
            dma((chunks, n_zb)),
            dma((chunks, n_zb)),
        ],
        compiler_params=pltpu.CompilerParams(
            collective_id=0, has_side_effects=True, vmem_limit_bytes=60 * 2**20
        ),
    )(source, *[jnp.asarray(t) for t in tables])
    part_x = lax.dynamic_slice_in_dim(symbol_x, lax.axis_index("ya") * kl, kl)
    part_y = lax.dynamic_slice_in_dim(symbol_y, lax.axis_index("zb") * jl, jl)
    symbol = part_x[:, None, None] + part_y[None, :, None] + symbol_z[None, None, :]
    return modes * lax.rsqrt(symbol)


def solution(mesh):
    placed = (P(None, "ya", "zb"), P(), P(), P())
    return jax.shard_map(
        functools.partial(body, mesh.shape["ya"], mesh.shape["zb"]),
        mesh=mesh, in_specs=placed, out_specs=P("ya", "zb", None), check_vma=False,
    )
```

```python
import functools

import jax
import jax.numpy as jnp
import numpy as np
from jax import lax
from jax.experimental import pallas as pl
from jax.experimental.pallas import tpu as pltpu
from jax.sharding import PartitionSpec as P

MESH = pl.DeviceIdType.MESH
AHEAD = 2
SHARES = (4,4,4,2,2)


def transform_table(count):
    rank = np.arange(1, count + 1)
    angle = np.pi / (count + 1) * (rank[:, None] * rank[None, :] % (2 * count + 2))
    table = np.sqrt(2.0 / (count + 1)) * np.sin(angle)
    high = table.astype(jnp.bfloat16)
    low = (table - high.astype(np.float64)).astype(jnp.bfloat16)
    return high, low


def halves(values):
    high = values.astype(jnp.bfloat16)
    return high, (values - high.astype(jnp.float32)).astype(jnp.bfloat16)


def left_product(table3, values):
    high, low = halves(values)
    stacked = jnp.concatenate([high, low, high], axis=0)
    return jnp.dot(table3, stacked, preferred_element_type=jnp.float32)


def partners(me, count):
    if count & (count - 1):
        return (
            [lax.rem(me + step, count) for step in range(count)],
            [lax.rem(me + count - step, count) for step in range(count)],
        )
    peers, bit = [me], 1
    while bit < count:
        turn = bit * (1 - 2 * lax.rem(lax.div(me, bit), 2))
        peers += [peer + turn for peer in peers]
        bit *= 2
    return peers, peers


def kernel(
    n_ya, n_zb, bounds,
    source, table_x, table_y, high_z, low_z, symbol_x, symbol_y, symbol_z,
    out,
    src, tx, ty, hz, lz, sx, sy, sz, first, second, third, lines, column_x, base,
    load_sem, send_a, recv_a, send_b, recv_b,
):
    ya, zb = lax.axis_index("ya"), lax.axis_index("zb")
    nx, yl, zl = source.shape
    ny = yl * n_ya
    kl = nx // n_ya
    jl = ny // n_zb
    nz = zl * n_zb
    chunks = len(bounds) - 1

    barrier = pltpu.get_barrier_semaphore()

    to_a, from_a = partners(ya, n_ya)
    to_b, from_b = partners(zb, n_zb)
    for axis, peers in (("ya", to_a), ("zb", to_b)):
        for peer in reversed(peers[1:]):
            pl.semaphore_signal(barrier, inc=1, device_id={axis: peer}, device_id_type=MESH)

    loads = [
        pltpu.make_async_copy(a, b, load_sem.at[i])
        for i, (a, b) in enumerate(
            [
                (source, src), (table_x, tx), (table_y, ty), (high_z, hz), (low_z, lz),
                (symbol_x, sx), (symbol_y, sy), (symbol_z, sz),
            ]
        )
    ]
    for load in loads:
        load.start()

    loads[0].wait()
    loads[1].wait()

    flat_src = src.reshape(nx * yl, zl)
    flat_first = first.reshape(nx * yl, zl)

    def x_step(pair, _):
        values = jnp.concatenate(
            [flat_src[pl.ds(2 * pair + t, nx, stride=yl), :] for t in range(2)], axis=1
        )
        modes = left_product(tx[...], values)
        for t in range(2):
            flat_first[pl.ds(2 * pair + t, nx, stride=yl), :] = modes[:, t * zl:(t + 1) * zl]
        return 0

    lax.fori_loop(0, yl // 2, x_step, 0)

    pl.semaphore_wait(barrier, n_ya + n_zb - 2)

    def size(chunk):
        return bounds[chunk + 1] - bounds[chunk]

    def span(chunk):
        return pl.ds(bounds[chunk], size(chunk))

    def copy_a(chunk, step):
        peer = to_a[step]
        return pltpu.make_async_remote_copy(
            src_ref=first.at[pl.ds(peer * kl + bounds[chunk], size(chunk))],
            dst_ref=second.at[span(chunk), pl.ds(pl.multiple_of(ya * yl, yl), yl)],
            send_sem=send_a.at[chunk, step],
            recv_sem=recv_a.at[chunk, step],
            device_id={"ya": peer},
            device_id_type=MESH,
        )

    def arrive_a(chunk, step):
        peer = from_a[step]
        there = second.at[span(chunk), pl.ds(pl.multiple_of(peer * yl, yl), yl)]
        return pltpu.make_async_copy(there, there, recv_a.at[chunk, step])

    def copy_b(chunk, step):
        peer = to_b[step]
        return pltpu.make_async_remote_copy(
            src_ref=third.at[span(chunk), pl.ds(pl.multiple_of(peer * jl, jl), jl)],
            dst_ref=lines.at[zb, span(chunk)],
            send_sem=send_b.at[chunk, step],
            recv_sem=recv_b.at[chunk, step],
            device_id={"zb": peer},
            device_id_type=MESH,
        )

    def arrive_b(chunk, step):
        there = lines.at[from_b[step], span(chunk)]
        return pltpu.make_async_copy(there, there, recv_b.at[chunk, step])

    def each_a(todo):
        for step in range(n_ya - 1, 0, -1):
            todo(step)

    def each_b(todo):
        for step in range(n_zb - 1, 0, -1):
            todo(step)

    for chunk in range(min(AHEAD, chunks)):
        each_a(lambda step: copy_a(chunk, step).start())

    second[:, pl.ds(pl.multiple_of(ya * yl, yl), yl), :] = first[pl.ds(ya * kl, kl)]

    for load in loads[2:]:
        load.wait()

    def column(row):
        return jnp.broadcast_to(row, (zl, row.shape[1])).T

    column_x[...] = column(sx[...])
    third[0] = column(sy[...])
    own_y = third[0, pl.ds(pl.multiple_of(zb * jl, jl), jl), :]
    base[...] = jnp.concatenate([own_y] * n_zb, axis=1) + sz[...]

    def y_stage(chunk):
        each_a(lambda step: arrive_a(chunk, step).wait())
        if chunk + AHEAD < chunks:
            each_a(lambda step: copy_a(chunk + AHEAD, step).start())
        for low in range(bounds[chunk], bounds[chunk + 1], 2):
            planes = range(low, min(low + 2, bounds[chunk + 1]))
            values = jnp.concatenate([second[k] for k in planes], axis=1)
            modes = left_product(ty[...], values)
            for t, k in enumerate(planes):
                third[k] = modes[:, t * zl:(t + 1) * zl]
        each_b(lambda step: copy_b(chunk, step).start())
        lines[zb, span(chunk)] = third[
            span(chunk), pl.ds(pl.multiple_of(zb * jl, jl), jl), :
        ]

    def z_stage(chunk):
        each_b(lambda step: arrive_b(chunk, step).wait())
        values = jnp.concatenate(
            [lines[b, span(chunk)].reshape(size(chunk) * jl, zl) for b in range(n_zb)], axis=1
        )
        high, low = halves(values)
        dot = functools.partial(jnp.dot, preferred_element_type=jnp.float32)
        modes = dot(high, hz[...]) + dot(low, hz[...]) + dot(high, lz[...])
        for t in range(size(chunk)):
            k = bounds[chunk] + t
            own_x = jnp.concatenate([column_x[pl.ds(ya * kl + k, 1), :]] * n_zb, axis=1)
            out[k] = modes[t * jl:(t + 1) * jl] * lax.rsqrt(base[...] + own_x)

    for chunk in range(chunks):
        y_stage(chunk)
        if chunk:
            z_stage(chunk - 1)
    z_stage(chunks - 1)

    for chunk in range(chunks):
        each_a(lambda step: copy_a(chunk, step).wait_send())
        each_b(lambda step: copy_b(chunk, step).wait_send())


def body(n_ya, n_zb, source, symbol_x, symbol_y, symbol_z):
    nx, yl, zl = source.shape
    ny, nz = yl * n_ya, zl * n_zb
    kl, jl = nx // n_ya, ny // n_zb
    ends = np.cumsum(SHARES) * kl // sum(SHARES)
    bounds = tuple(sorted({0, *ends.tolist()}))
    chunks = len(bounds) - 1
    tables = []
    for count in (nx, ny):
        high, low = transform_table(count)
        tables.append(np.concatenate([high, high, low], axis=1))
    tables += list(transform_table(nz))
    room = 67_043_328 - 4 * kl * jl * nz - 2**18
    dma = pltpu.SemaphoreType.DMA
    vmem = pltpu.VMEM
    return pl.pallas_call(
        functools.partial(kernel, n_ya, n_zb, bounds),
        out_shape=pltpu.VMEM((kl, jl, nz), jnp.float32),
        in_specs=[pl.BlockSpec(memory_space=pltpu.HBM)] * 8,
        out_specs=pl.BlockSpec(memory_space=pltpu.VMEM),
        scratch_shapes=[
            vmem((nx, yl, zl), jnp.float32),
            vmem((nx, 3 * nx), jnp.bfloat16),
            vmem((ny, 3 * ny), jnp.bfloat16),
            vmem((nz, nz), jnp.bfloat16),
            vmem((nz, nz), jnp.bfloat16),
            vmem((1, nx), jnp.float32),
            vmem((1, ny), jnp.float32),
            vmem((1, nz), jnp.float32),
            vmem((nx, yl, zl), jnp.float32),
            vmem((kl, ny, zl), jnp.float32),
            vmem((kl, ny, zl), jnp.float32),
            vmem((n_zb, kl, jl, zl), jnp.float32),
            vmem((nx, zl), jnp.float32),
            vmem((jl, nz), jnp.float32),
            dma((8,)),
            dma((chunks, n_ya)),
            dma((chunks, n_ya)),
            dma((chunks, n_zb)),
            dma((chunks, n_zb)),
        ],
        compiler_params=pltpu.CompilerParams(
            collective_id=0, has_side_effects=True, vmem_limit_bytes=room
        ),
    )(
        source, *[jnp.asarray(t) for t in tables],
        symbol_x[None], symbol_y[None], symbol_z[None],
    )


def solution(mesh):
    placed = (P(None, "ya", "zb"), P(), P(), P())
    return jax.shard_map(
        functools.partial(body, mesh.shape["ya"], mesh.shape["zb"]),
        mesh=mesh, in_specs=placed, out_specs=P("ya", "zb", None), check_vma=False,
    )
```

```python
import functools

import jax
import jax.numpy as jnp
import numpy as np
from jax import lax
from jax.experimental import pallas as pl
from jax.experimental.pallas import tpu as pltpu
from jax.sharding import PartitionSpec as P

MESH = pl.DeviceIdType.MESH
AHEAD = 2
SHARES = (5,5,4,2)


def transform_table(count):
    rank = np.arange(1, count + 1)
    angle = np.pi / (count + 1) * (rank[:, None] * rank[None, :] % (2 * count + 2))
    table = np.sqrt(2.0 / (count + 1)) * np.sin(angle)
    high = table.astype(jnp.bfloat16)
    low = (table - high.astype(np.float64)).astype(jnp.bfloat16)
    return high, low


def halves(values):
    high = values.astype(jnp.bfloat16)
    return high, (values - high.astype(jnp.float32)).astype(jnp.bfloat16)


def left_product(table3, values):
    high, low = halves(values)
    stacked = jnp.concatenate([high, low, high], axis=0)
    return jnp.dot(table3, stacked, preferred_element_type=jnp.float32)


def partners(me, count):
    if count & (count - 1):
        return (
            [lax.rem(me + step, count) for step in range(count)],
            [lax.rem(me + count - step, count) for step in range(count)],
        )
    peers, bit = [me], 1
    while bit < count:
        turn = bit * (1 - 2 * lax.rem(lax.div(me, bit), 2))
        peers += [peer + turn for peer in peers]
        bit *= 2
    return peers, peers


def kernel(
    n_ya, n_zb, bounds,
    source, table_x, table_y, high_z, low_z, symbol_x, symbol_y, symbol_z,
    out,
    src, tx, ty, hz, lz, sx, sy, sz, first, second, third, lines, column_x, base,
    load_sem, met, send_a, recv_a, send_b, recv_b,
):
    ya, zb = lax.axis_index("ya"), lax.axis_index("zb")
    nx, yl, zl = source.shape
    ny = yl * n_ya
    kl = nx // n_ya
    jl = ny // n_zb
    nz = zl * n_zb
    chunks = len(bounds) - 1

    barrier = pltpu.get_barrier_semaphore()

    to_a, from_a = partners(ya, n_ya)
    to_b, from_b = partners(zb, n_zb)
    paired = n_ya & (n_ya - 1) == 0
    direct = [step for step in range(1, n_ya) if not paired or step & (step - 1) == 0]
    rounds = len(direct) - 1 if paired else 0
    greeted = [("ya", to_a[step]) for step in reversed(direct)] + [("zb", peer) for peer in to_b[1:]]
    for axis, peer in greeted:
        pl.semaphore_signal(barrier, inc=1, device_id={axis: peer}, device_id_type=MESH)

    loads = [
        pltpu.make_async_copy(a, b, load_sem.at[i])
        for i, (a, b) in enumerate(
            [
                (source, src), (table_x, tx), (table_y, ty), (high_z, hz), (low_z, lz),
                (symbol_x, sx), (symbol_y, sy), (symbol_z, sz),
            ]
        )
    ]
    for load in loads:
        load.start()

    loads[0].wait()
    loads[1].wait()

    def tell(turn):
        if turn < rounds:
            pl.semaphore_signal(
                met.at[turn], inc=1, device_id={"ya": to_a[2**turn]}, device_id_type=MESH
            )

    flat_src = src.reshape(nx * yl, zl)
    flat_first = first.reshape(nx * yl, zl)

    def x_step(pair, _):
        values = jnp.concatenate(
            [flat_src[pl.ds(2 * pair + t, nx, stride=yl), :] for t in range(2)], axis=1
        )
        modes = left_product(tx[...], values)
        for t in range(2):
            flat_first[pl.ds(2 * pair + t, nx, stride=yl), :] = modes[:, t * zl:(t + 1) * zl]
        return 0

    lax.fori_loop(0, yl // 2, x_step, 0, unroll=8)

    pl.semaphore_wait(barrier, len(greeted))
    tell(0)

    def size(chunk):
        return bounds[chunk + 1] - bounds[chunk]

    def span(chunk):
        return pl.ds(bounds[chunk], size(chunk))

    def copy_a(chunk, step):
        peer = to_a[step]
        return pltpu.make_async_remote_copy(
            src_ref=first.at[pl.ds(peer * kl + bounds[chunk], size(chunk))],
            dst_ref=second.at[span(chunk), pl.ds(pl.multiple_of(ya * yl, yl), yl)],
            send_sem=send_a.at[chunk, step],
            recv_sem=recv_a.at[chunk, step],
            device_id={"ya": peer},
            device_id_type=MESH,
        )

    def arrive_a(chunk, step):
        peer = from_a[step]
        there = second.at[span(chunk), pl.ds(pl.multiple_of(peer * yl, yl), yl)]
        return pltpu.make_async_copy(there, there, recv_a.at[chunk, step])

    def copy_b(chunk, step):
        peer = to_b[step]
        return pltpu.make_async_remote_copy(
            src_ref=third.at[span(chunk), pl.ds(pl.multiple_of(peer * jl, jl), jl)],
            dst_ref=lines.at[zb, span(chunk)],
            send_sem=send_b.at[chunk, step],
            recv_sem=recv_b.at[chunk, step],
            device_id={"zb": peer},
            device_id_type=MESH,
        )

    def arrive_b(chunk, step):
        there = lines.at[from_b[step], span(chunk)]
        return pltpu.make_async_copy(there, there, recv_b.at[chunk, step])

    order = [*range(n_ya // 2, n_ya), *range(n_ya // 2 - 1, 0, -1)]

    def each_a(todo):
        for step in order:
            todo(step)

    def each_b(todo):
        for step in range(n_zb - 1, 0, -1):
            todo(step)

    heard = 0
    for step in order:
        need = (step - 2 ** (step.bit_length() - 1)).bit_length() if paired else 0
        while heard < need:
            pl.semaphore_wait(met.at[heard], 1)
            heard += 1
            tell(heard)
        copy_a(0, step).start()
    while heard < rounds:
        pl.semaphore_wait(met.at[heard], 1)
        heard += 1
        tell(heard)
    for chunk in range(1, min(AHEAD, chunks)):
        each_a(lambda step: copy_a(chunk, step).start())

    second[:, pl.ds(pl.multiple_of(ya * yl, yl), yl), :] = first[pl.ds(ya * kl, kl)]

    for load in loads[2:]:
        load.wait()

    def column(row):
        return jnp.broadcast_to(row, (zl, row.shape[1])).T

    column_x[...] = column(sx[...])
    third[0] = column(sy[...])
    own_y = third[0, pl.ds(pl.multiple_of(zb * jl, jl), jl), :]
    base[...] = jnp.concatenate([own_y] * n_zb, axis=1) + sz[...]

    def y_stage(chunk):
        each_a(lambda step: arrive_a(chunk, step).wait())
        if chunk + AHEAD < chunks:
            each_a(lambda step: copy_a(chunk + AHEAD, step).start())
        for low in range(bounds[chunk], bounds[chunk + 1], 2):
            planes = range(low, min(low + 2, bounds[chunk + 1]))
            values = jnp.concatenate([second[k] for k in planes], axis=1)
            modes = left_product(ty[...], values)
            for t, k in enumerate(planes):
                third[k] = modes[:, t * zl:(t + 1) * zl]
        each_b(lambda step: copy_b(chunk, step).start())
        lines[zb, span(chunk)] = third[
            span(chunk), pl.ds(pl.multiple_of(zb * jl, jl), jl), :
        ]

    def z_stage(chunk):
        each_b(lambda step: arrive_b(chunk, step).wait())
        values = jnp.concatenate(
            [lines[b, span(chunk)].reshape(size(chunk) * jl, zl) for b in range(n_zb)], axis=1
        )
        high, low = halves(values)
        dot = functools.partial(jnp.dot, preferred_element_type=jnp.float32)
        modes = dot(high, hz[...]) + dot(low, hz[...]) + dot(high, lz[...])
        for t in range(size(chunk)):
            k = bounds[chunk] + t
            own_x = jnp.concatenate([column_x[pl.ds(ya * kl + k, 1), :]] * n_zb, axis=1)
            out[k] = modes[t * jl:(t + 1) * jl] * lax.rsqrt(base[...] + own_x)

    for chunk in range(chunks):
        y_stage(chunk)
        if chunk:
            z_stage(chunk - 1)
    z_stage(chunks - 1)

    for chunk in range(chunks):
        each_a(lambda step: copy_a(chunk, step).wait_send())
        each_b(lambda step: copy_b(chunk, step).wait_send())


def body(n_ya, n_zb, source, symbol_x, symbol_y, symbol_z):
    nx, yl, zl = source.shape
    ny, nz = yl * n_ya, zl * n_zb
    kl, jl = nx // n_ya, ny // n_zb
    ends = np.cumsum(SHARES) * kl // sum(SHARES)
    bounds = tuple(sorted({0, *ends.tolist()}))
    chunks = len(bounds) - 1
    tables = []
    for count in (nx, ny):
        high, low = transform_table(count)
        tables.append(np.concatenate([high, high, low], axis=1))
    tables += list(transform_table(nz))
    room = 67_043_328 - 4 * kl * jl * nz - 2**18
    dma = pltpu.SemaphoreType.DMA
    vmem = pltpu.VMEM
    return pl.pallas_call(
        functools.partial(kernel, n_ya, n_zb, bounds),
        out_shape=pltpu.VMEM((kl, jl, nz), jnp.float32),
        in_specs=[pl.BlockSpec(memory_space=pltpu.HBM)] * 8,
        out_specs=pl.BlockSpec(memory_space=pltpu.VMEM),
        scratch_shapes=[
            vmem((nx, yl, zl), jnp.float32),
            vmem((nx, 3 * nx), jnp.bfloat16),
            vmem((ny, 3 * ny), jnp.bfloat16),
            vmem((nz, nz), jnp.bfloat16),
            vmem((nz, nz), jnp.bfloat16),
            vmem((1, nx), jnp.float32),
            vmem((1, ny), jnp.float32),
            vmem((1, nz), jnp.float32),
            vmem((nx, yl, zl), jnp.float32),
            vmem((kl, ny, zl), jnp.float32),
            vmem((kl, ny, zl), jnp.float32),
            vmem((n_zb, kl, jl, zl), jnp.float32),
            vmem((nx, zl), jnp.float32),
            vmem((jl, nz), jnp.float32),
            dma((8,)),
            pltpu.SemaphoreType.REGULAR((max(1, n_ya.bit_length() - 2),)),
            dma((chunks, n_ya)),
            dma((chunks, n_ya)),
            dma((chunks, n_zb)),
            dma((chunks, n_zb)),
        ],
        compiler_params=pltpu.CompilerParams(
            collective_id=0, has_side_effects=True, vmem_limit_bytes=room
        ),
    )(
        source, *[jnp.asarray(t) for t in tables],
        symbol_x[None], symbol_y[None], symbol_z[None],
    )


def solution(mesh):
    placed = (P(None, "ya", "zb"), P(), P(), P())
    return jax.shard_map(
        functools.partial(body, mesh.shape["ya"], mesh.shape["zb"]),
        mesh=mesh, in_specs=placed, out_specs=P("ya", "zb", None), check_vma=False,
    )
```

```python
import functools

import jax
import jax.numpy as jnp
import numpy as np
from jax import lax
from jax.experimental import pallas as pl
from jax.experimental.pallas import tpu as pltpu
from jax.sharding import PartitionSpec as P

MESH = pl.DeviceIdType.MESH
AHEAD = 2
SHARES = (5,5,4,2)


def transform_table(count):
    rank = np.arange(1, count + 1)
    angle = np.pi / (count + 1) * (rank[:, None] * rank[None, :] % (2 * count + 2))
    table = np.sqrt(2.0 / (count + 1)) * np.sin(angle)
    high = table.astype(jnp.bfloat16)
    low = (table - high.astype(np.float64)).astype(jnp.bfloat16)
    return high, low


def halves(values):
    high = values.astype(jnp.bfloat16)
    return high, (values - high.astype(jnp.float32)).astype(jnp.bfloat16)


def left_product(table3, values):
    high, low = halves(values)
    stacked = jnp.concatenate([high, low, high], axis=0)
    return jnp.dot(table3, stacked, preferred_element_type=jnp.float32)


def partners(me, count):
    if count & (count - 1):
        return (
            [lax.rem(me + step, count) for step in range(count)],
            [lax.rem(me + count - step, count) for step in range(count)],
        )
    peers, bit = [me], 1
    while bit < count:
        turn = bit * (1 - 2 * lax.rem(lax.div(me, bit), 2))
        peers += [peer + turn for peer in peers]
        bit *= 2
    return peers, peers


def kernel(
    n_ya, n_zb, bounds,
    source, table_x, table_y, high_z, low_z, symbol_x, symbol_y, symbol_z,
    out,
    src, tx, ty, hz, lz, sx, sy, sz, first, second, third, lines, column_x, base,
    load_sem, met, send_a, recv_a, send_b, recv_b,
):
    ya, zb = lax.axis_index("ya"), lax.axis_index("zb")
    nx, yl, zl = source.shape
    ny = yl * n_ya
    kl = nx // n_ya
    jl = ny // n_zb
    nz = zl * n_zb
    chunks = len(bounds) - 1

    barrier = pltpu.get_barrier_semaphore()

    to_a, from_a = partners(ya, n_ya)
    to_b, from_b = partners(zb, n_zb)
    paired = n_ya & (n_ya - 1) == 0
    direct = [step for step in range(1, n_ya) if not paired or step & (step - 1) == 0]
    rounds = len(direct) - 1 if paired else 0
    greeted = [("ya", to_a[step]) for step in reversed(direct)] + [("zb", peer) for peer in to_b[1:]]
    for axis, peer in greeted:
        pl.semaphore_signal(barrier, inc=1, device_id={axis: peer}, device_id_type=MESH)

    rows = 8 if yl % 8 == 0 else yl
    parts = [pl.ds(row, rows) for row in range(0, yl, rows)]
    loads = [
        pltpu.make_async_copy(a, b, load_sem.at[i])
        for i, (a, b) in enumerate(
            [
                (table_x, tx),
                *[(source.at[:, part], src.at[:, part]) for part in parts],
                (table_y, ty), (high_z, hz), (low_z, lz),
                (symbol_x, sx), (symbol_y, sy), (symbol_z, sz),
            ]
        )
    ]
    for load in loads:
        load.start()

    loads[0].wait()

    def tell(turn):
        if turn < rounds:
            pl.semaphore_signal(
                met.at[turn], inc=1, device_id={"ya": to_a[2**turn]}, device_id_type=MESH
            )

    flat_src = src.reshape(nx * yl, zl)
    flat_first = first.reshape(nx * yl, zl)

    def x_step(pair, _):
        values = jnp.concatenate(
            [flat_src[pl.ds(2 * pair + t, nx, stride=yl), :] for t in range(2)], axis=1
        )
        modes = left_product(tx[...], values)
        for t in range(2):
            flat_first[pl.ds(2 * pair + t, nx, stride=yl), :] = modes[:, t * zl:(t + 1) * zl]
        return 0

    for i in range(len(parts)):
        loads[1 + i].wait()
        lax.fori_loop(i * rows // 2, (i + 1) * rows // 2, x_step, 0, unroll=rows // 2)

    pl.semaphore_wait(barrier, len(greeted))
    tell(0)

    def size(chunk):
        return bounds[chunk + 1] - bounds[chunk]

    def span(chunk):
        return pl.ds(bounds[chunk], size(chunk))

    def copy_a(chunk, step):
        peer = to_a[step]
        return pltpu.make_async_remote_copy(
            src_ref=first.at[pl.ds(peer * kl + bounds[chunk], size(chunk))],
            dst_ref=second.at[span(chunk), pl.ds(pl.multiple_of(ya * yl, yl), yl)],
            send_sem=send_a.at[chunk, step],
            recv_sem=recv_a.at[chunk, step],
            device_id={"ya": peer},
            device_id_type=MESH,
        )

    def arrive_a(chunk, step):
        peer = from_a[step]
        there = second.at[span(chunk), pl.ds(pl.multiple_of(peer * yl, yl), yl)]
        return pltpu.make_async_copy(there, there, recv_a.at[chunk, step])

    def copy_b(chunk, step):
        peer = to_b[step]
        return pltpu.make_async_remote_copy(
            src_ref=third.at[span(chunk), pl.ds(pl.multiple_of(peer * jl, jl), jl)],
            dst_ref=lines.at[zb, span(chunk)],
            send_sem=send_b.at[chunk, step],
            recv_sem=recv_b.at[chunk, step],
            device_id={"zb": peer},
            device_id_type=MESH,
        )

    def arrive_b(chunk, step):
        there = lines.at[from_b[step], span(chunk)]
        return pltpu.make_async_copy(there, there, recv_b.at[chunk, step])

    order = [*range(n_ya // 2, n_ya), *range(n_ya // 2 - 1, 0, -1)]

    later = [*range(n_ya // 2 - 1, 0, -1), *range(n_ya // 2, n_ya)]

    def each_a(todo, steps=None):
        for step in steps or order:
            todo(step)

    def each_b(todo):
        for step in range(n_zb - 1, 0, -1):
            todo(step)

    heard = 0
    for step in order:
        need = (step - 2 ** (step.bit_length() - 1)).bit_length() if paired else 0
        while heard < need:
            pl.semaphore_wait(met.at[heard], 1)
            heard += 1
            tell(heard)
        copy_a(0, step).start()
    while heard < rounds:
        pl.semaphore_wait(met.at[heard], 1)
        heard += 1
        tell(heard)
    for chunk in range(1, min(AHEAD, chunks)):
        each_a(lambda step: copy_a(chunk, step).start(), later)

    second[:, pl.ds(pl.multiple_of(ya * yl, yl), yl), :] = first[pl.ds(ya * kl, kl)]

    for load in loads[1 + len(parts):]:
        load.wait()

    def column(row):
        return jnp.broadcast_to(row, (zl, row.shape[1])).T

    column_x[...] = column(sx[...])
    third[0] = column(sy[...])
    own_y = third[0, pl.ds(pl.multiple_of(zb * jl, jl), jl), :]
    base[...] = jnp.concatenate([own_y] * n_zb, axis=1) + sz[...]

    def y_stage(chunk):
        each_a(lambda step: arrive_a(chunk, step).wait())
        for low in range(bounds[chunk], bounds[chunk + 1], 2):
            planes = range(low, min(low + 2, bounds[chunk + 1]))
            values = jnp.concatenate([second[k] for k in planes], axis=1)
            modes = left_product(ty[...], values)
            for t, k in enumerate(planes):
                third[k] = modes[:, t * zl:(t + 1) * zl]
        each_b(lambda step: copy_b(chunk, step).start())
        if chunk + AHEAD < chunks:
            each_a(lambda step: copy_a(chunk + AHEAD, step).start(), later)
        lines[zb, span(chunk)] = third[
            span(chunk), pl.ds(pl.multiple_of(zb * jl, jl), jl), :
        ]

    def z_stage(chunk):
        each_b(lambda step: arrive_b(chunk, step).wait())
        values = jnp.concatenate(
            [lines[b, span(chunk)].reshape(size(chunk) * jl, zl) for b in range(n_zb)], axis=1
        )
        high, low = halves(values)
        dot = functools.partial(jnp.dot, preferred_element_type=jnp.float32)
        modes = dot(high, hz[...]) + dot(low, hz[...]) + dot(high, lz[...])
        for t in range(size(chunk)):
            k = bounds[chunk] + t
            own_x = jnp.concatenate([column_x[pl.ds(ya * kl + k, 1), :]] * n_zb, axis=1)
            out[k] = modes[t * jl:(t + 1) * jl] * lax.rsqrt(base[...] + own_x)

    for chunk in range(chunks):
        y_stage(chunk)
        if chunk:
            z_stage(chunk - 1)
    z_stage(chunks - 1)

    for chunk in range(chunks):
        each_a(lambda step: copy_a(chunk, step).wait_send())
        each_b(lambda step: copy_b(chunk, step).wait_send())


def body(n_ya, n_zb, source, symbol_x, symbol_y, symbol_z):
    nx, yl, zl = source.shape
    ny, nz = yl * n_ya, zl * n_zb
    kl, jl = nx // n_ya, ny // n_zb
    ends = np.cumsum(SHARES) * kl // sum(SHARES)
    bounds = tuple(sorted({0, *ends.tolist()}))
    chunks = len(bounds) - 1
    tables = []
    for count in (nx, ny):
        high, low = transform_table(count)
        tables.append(np.concatenate([high, high, low], axis=1))
    tables += list(transform_table(nz))
    room = 67_043_328 - 4 * kl * jl * nz - 2**18
    dma = pltpu.SemaphoreType.DMA
    vmem = pltpu.VMEM
    return pl.pallas_call(
        functools.partial(kernel, n_ya, n_zb, bounds),
        out_shape=pltpu.VMEM((kl, jl, nz), jnp.float32),
        in_specs=[pl.BlockSpec(memory_space=pltpu.HBM)] * 8,
        out_specs=pl.BlockSpec(memory_space=pltpu.VMEM),
        scratch_shapes=[
            vmem((nx, yl, zl), jnp.float32),
            vmem((nx, 3 * nx), jnp.bfloat16),
            vmem((ny, 3 * ny), jnp.bfloat16),
            vmem((nz, nz), jnp.bfloat16),
            vmem((nz, nz), jnp.bfloat16),
            vmem((1, nx), jnp.float32),
            vmem((1, ny), jnp.float32),
            vmem((1, nz), jnp.float32),
            vmem((nx, yl, zl), jnp.float32),
            vmem((kl, ny, zl), jnp.float32),
            vmem((kl, ny, zl), jnp.float32),
            vmem((n_zb, kl, jl, zl), jnp.float32),
            vmem((nx, zl), jnp.float32),
            vmem((jl, nz), jnp.float32),
            dma((7 + max(1, yl // 8),)),
            pltpu.SemaphoreType.REGULAR((max(1, n_ya.bit_length() - 2),)),
            dma((chunks, n_ya)),
            dma((chunks, n_ya)),
            dma((chunks, n_zb)),
            dma((chunks, n_zb)),
        ],
        compiler_params=pltpu.CompilerParams(
            collective_id=0, has_side_effects=True, vmem_limit_bytes=room
        ),
    )(
        source, *[jnp.asarray(t) for t in tables],
        symbol_x[None], symbol_y[None], symbol_z[None],
    )


def solution(mesh):
    placed = (P(None, "ya", "zb"), P(), P(), P())
    return jax.shard_map(
        functools.partial(body, mesh.shape["ya"], mesh.shape["zb"]),
        mesh=mesh, in_specs=placed, out_specs=P("ya", "zb", None), check_vma=False,
    )
```

```python
import functools

import jax
import jax.numpy as jnp
import numpy as np
from jax import lax
from jax.experimental import pallas as pl
from jax.experimental.pallas import tpu as pltpu
from jax.sharding import PartitionSpec as P

MESH = pl.DeviceIdType.MESH
AHEAD = 2
SHARES = (5,5,4,2)


def transform_table(count):
    rank = np.arange(1, count + 1)
    angle = np.pi / (count + 1) * (rank[:, None] * rank[None, :] % (2 * count + 2))
    table = np.sqrt(2.0 / (count + 1)) * np.sin(angle)
    high = table.astype(jnp.bfloat16)
    low = (table - high.astype(np.float64)).astype(jnp.bfloat16)
    return high, low


def halves(values):
    high = values.astype(jnp.bfloat16)
    return high, (values - high.astype(jnp.float32)).astype(jnp.bfloat16)


def left_product(table3, values):
    high, low = halves(values)
    stacked = jnp.concatenate([high, low, high], axis=0)
    return jnp.dot(table3, stacked, preferred_element_type=jnp.float32)


def partners(me, count):
    if count & (count - 1):
        return (
            [lax.rem(me + step, count) for step in range(count)],
            [lax.rem(me + count - step, count) for step in range(count)],
        )
    peers, bit = [me], 1
    while bit < count:
        turn = bit * (1 - 2 * lax.rem(lax.div(me, bit), 2))
        peers += [peer + turn for peer in peers]
        bit *= 2
    return peers, peers


def kernel(
    n_ya, n_zb, bounds,
    source, table_x, table_y, high_z, low_z, symbol_x, symbol_y, symbol_z,
    out,
    src, tx, ty, hz, lz, sx, sy, sz, first, second, third, lines, column_x, base,
    load_sem, met, send_a, recv_a, send_b, recv_b,
):
    ya, zb = lax.axis_index("ya"), lax.axis_index("zb")
    nx, yl, zl = source.shape
    ny = yl * n_ya
    kl = nx // n_ya
    jl = ny // n_zb
    nz = zl * n_zb
    chunks = len(bounds) - 1

    barrier = pltpu.get_barrier_semaphore()

    to_a, from_a = partners(ya, n_ya)
    to_b, from_b = partners(zb, n_zb)
    paired = n_ya & (n_ya - 1) == 0
    direct = [step for step in range(1, n_ya) if not paired or step & (step - 1) == 0]
    rounds = len(direct) - 1 if paired else 0
    greeted = [("ya", to_a[step]) for step in reversed(direct)] + [("zb", peer) for peer in to_b[1:]]
    for axis, peer in greeted:
        pl.semaphore_signal(barrier, inc=1, device_id={axis: peer}, device_id_type=MESH)

    loads = [
        pltpu.make_async_copy(a, b, load_sem.at[i])
        for i, (a, b) in enumerate(
            [
                (source, src), (table_x, tx), (table_y, ty), (high_z, hz), (low_z, lz),
                (symbol_x, sx), (symbol_y, sy), (symbol_z, sz),
            ]
        )
    ]
    for load in loads:
        load.start()

    loads[0].wait()
    loads[1].wait()

    def tell(turn):
        if turn < rounds:
            pl.semaphore_signal(
                met.at[turn], inc=1, device_id={"ya": to_a[2**turn]}, device_id_type=MESH
            )

    flat_src = src.reshape(nx * yl, zl)
    flat_first = first.reshape(nx * yl, zl)

    def x_step(pair, _):
        values = jnp.concatenate(
            [flat_src[pl.ds(2 * pair + t, nx, stride=yl), :] for t in range(2)], axis=1
        )
        modes = left_product(tx[...], values)
        for t in range(2):
            flat_first[pl.ds(2 * pair + t, nx, stride=yl), :] = modes[:, t * zl:(t + 1) * zl]
        return 0

    lax.fori_loop(0, yl // 2, x_step, 0, unroll=8)

    pl.semaphore_wait(barrier, len(greeted))
    tell(0)

    def size(chunk):
        return bounds[chunk + 1] - bounds[chunk]

    def span(chunk):
        return pl.ds(bounds[chunk], size(chunk))

    def copy_a(chunk, step):
        peer = to_a[step]
        return pltpu.make_async_remote_copy(
            src_ref=first.at[pl.ds(peer * kl + bounds[chunk], size(chunk))],
            dst_ref=second.at[span(chunk), pl.ds(pl.multiple_of(ya * yl, yl), yl)],
            send_sem=send_a.at[chunk, step],
            recv_sem=recv_a.at[chunk, step],
            device_id={"ya": peer},
            device_id_type=MESH,
        )

    def arrive_a(chunk, step):
        peer = from_a[step]
        there = second.at[span(chunk), pl.ds(pl.multiple_of(peer * yl, yl), yl)]
        return pltpu.make_async_copy(there, there, recv_a.at[chunk, step])

    def copy_b(chunk, step):
        peer = to_b[step]
        return pltpu.make_async_remote_copy(
            src_ref=third.at[span(chunk), pl.ds(pl.multiple_of(peer * jl, jl), jl)],
            dst_ref=lines.at[zb, span(chunk)],
            send_sem=send_b.at[chunk, step],
            recv_sem=recv_b.at[chunk, step],
            device_id={"zb": peer},
            device_id_type=MESH,
        )

    def arrive_b(chunk, step):
        there = lines.at[from_b[step], span(chunk)]
        return pltpu.make_async_copy(there, there, recv_b.at[chunk, step])

    order = [*range(n_ya // 2, n_ya), *range(n_ya // 2 - 1, 0, -1)]

    def each_a(todo):
        for step in order:
            todo(step)

    def each_b(todo):
        for step in range(n_zb - 1, 0, -1):
            todo(step)

    heard = 0
    for step in order:
        need = (step - 2 ** (step.bit_length() - 1)).bit_length() if paired else 0
        while heard < need:
            pl.semaphore_wait(met.at[heard], 1)
            heard += 1
            tell(heard)
        copy_a(0, step).start()
    while heard < rounds:
        pl.semaphore_wait(met.at[heard], 1)
        heard += 1
        tell(heard)
    for chunk in range(1, min(AHEAD, chunks)):
        each_a(lambda step: copy_a(chunk, step).start())

    second[:, pl.ds(pl.multiple_of(ya * yl, yl), yl), :] = first[pl.ds(ya * kl, kl)]

    for load in loads[2:]:
        load.wait()

    def column(row):
        return jnp.broadcast_to(row, (zl, row.shape[1])).T

    column_x[...] = column(sx[...])
    third[0] = column(sy[...])
    own_y = third[0, pl.ds(pl.multiple_of(zb * jl, jl), jl), :]
    base[...] = jnp.concatenate([own_y] * n_zb, axis=1) + sz[...]

    def y_stage(chunk):
        each_a(lambda step: arrive_a(chunk, step).wait())
        if chunk + AHEAD < chunks:
            each_a(lambda step: copy_a(chunk + AHEAD, step).start())
        for low in range(bounds[chunk], bounds[chunk + 1], 2):
            planes = range(low, min(low + 2, bounds[chunk + 1]))
            values = jnp.concatenate([second[k] for k in planes], axis=1)
            modes = left_product(ty[...], values)
            for t, k in enumerate(planes):
                third[k] = modes[:, t * zl:(t + 1) * zl]
        each_b(lambda step: copy_b(chunk, step).start())
        lines[zb, span(chunk)] = third[
            span(chunk), pl.ds(pl.multiple_of(zb * jl, jl), jl), :
        ]

    def z_stage(chunk):
        each_b(lambda step: arrive_b(chunk, step).wait())
        values = jnp.concatenate(
            [lines[b, span(chunk)].reshape(size(chunk) * jl, zl) for b in range(n_zb)], axis=1
        )
        high, low = halves(values)
        dot = functools.partial(jnp.dot, preferred_element_type=jnp.float32)
        both = dot(jnp.concatenate([high, low], axis=0), hz[...])
        rows = high.shape[0]
        modes = both[:rows] + both[rows:] + dot(high, lz[...])
        for t in range(size(chunk)):
            k = bounds[chunk] + t
            own_x = jnp.concatenate([column_x[pl.ds(ya * kl + k, 1), :]] * n_zb, axis=1)
            out[k] = modes[t * jl:(t + 1) * jl] * lax.rsqrt(base[...] + own_x)

    for chunk in range(chunks):
        y_stage(chunk)
        if chunk:
            z_stage(chunk - 1)
    z_stage(chunks - 1)

    for chunk in range(chunks):
        each_a(lambda step: copy_a(chunk, step).wait_send())
        each_b(lambda step: copy_b(chunk, step).wait_send())


def body(n_ya, n_zb, source, symbol_x, symbol_y, symbol_z):
    nx, yl, zl = source.shape
    ny, nz = yl * n_ya, zl * n_zb
    kl, jl = nx // n_ya, ny // n_zb
    ends = np.cumsum(SHARES) * kl // sum(SHARES)
    bounds = tuple(sorted({0, *ends.tolist()}))
    chunks = len(bounds) - 1
    tables = []
    for count in (nx, ny):
        high, low = transform_table(count)
        tables.append(np.concatenate([high, high, low], axis=1))
    tables += list(transform_table(nz))
    room = 67_043_328 - 4 * kl * jl * nz - 2**18
    dma = pltpu.SemaphoreType.DMA
    vmem = pltpu.VMEM
    return pl.pallas_call(
        functools.partial(kernel, n_ya, n_zb, bounds),
        out_shape=pltpu.VMEM((kl, jl, nz), jnp.float32),
        in_specs=[pl.BlockSpec(memory_space=pltpu.HBM)] * 8,
        out_specs=pl.BlockSpec(memory_space=pltpu.VMEM),
        scratch_shapes=[
            vmem((nx, yl, zl), jnp.float32),
            vmem((nx, 3 * nx), jnp.bfloat16),
            vmem((ny, 3 * ny), jnp.bfloat16),
            vmem((nz, nz), jnp.bfloat16),
            vmem((nz, nz), jnp.bfloat16),
            vmem((1, nx), jnp.float32),
            vmem((1, ny), jnp.float32),
            vmem((1, nz), jnp.float32),
            vmem((nx, yl, zl), jnp.float32),
            vmem((kl, ny, zl), jnp.float32),
            vmem((kl, ny, zl), jnp.float32),
            vmem((n_zb, kl, jl, zl), jnp.float32),
            vmem((nx, zl), jnp.float32),
            vmem((jl, nz), jnp.float32),
            dma((8,)),
            pltpu.SemaphoreType.REGULAR((max(1, n_ya.bit_length() - 2),)),
            dma((chunks, n_ya)),
            dma((chunks, n_ya)),
            dma((chunks, n_zb)),
            dma((chunks, n_zb)),
        ],
        compiler_params=pltpu.CompilerParams(
            collective_id=0, has_side_effects=True, vmem_limit_bytes=room
        ),
    )(
        source, *[jnp.asarray(t) for t in tables],
        symbol_x[None], symbol_y[None], symbol_z[None],
    )


def solution(mesh):
    placed = (P(None, "ya", "zb"), P(), P(), P())
    return jax.shard_map(
        functools.partial(body, mesh.shape["ya"], mesh.shape["zb"]),
        mesh=mesh, in_specs=placed, out_specs=P("ya", "zb", None), check_vma=False,
    )
```
